32 devices in a mesh: wa: 8 (over y, x, core), ch: 4 (over z).
Axes of the slice: x: 2, y: 2, z: 4, core: 2. Of those that a mesh axis runs over, the one named last changes fastest.
Arguments:
- grid_cells: int32 [2, 16384], P(None, ('wa', 'ch')), may hold values from -4096 to 4095
- visibilities: float32 [2, 16384], P(None, ('wa', 'ch')), may hold values from -6 to 6
- weights: float32 [16384], P(('wa', 'ch')), may hold values from 0.25 to 4
- layer_index: int32 [16384], P(('wa', 'ch')), may hold values from 0 to 7, as said below
- group_index: int32 [16384], P(('wa', 'ch')), may hold values from 0 to 3, as said below
- plane_depths: float32 [8], P('wa'), may hold values from -1000 to 1000
- sky_model: float32 [4, 128, 4096], P('ch', 'wa'), may hold values from -6 to 6
Outputs:
- residual: float32 [4, 128, 4096], P('ch', 'wa')
The draws below stay inside these ranges and needn't reach their ends.
Inputs may be any that keep to these rules, and one draw needn't show every extreme that they name: `layer_index`: among the 512 visibilities of one device, at most 32 have the same layer and the same group; one layer and group has exactly 32 on every device. `group_index`: drawn together with layer_index.
All inputs are finite; a program needn't handle non-finite values.
Results may differ from the reference program's by a relative error of at most 0.0026.
Values sent between devices are 32-bit elements; how exact they have to be, the bound alone decides.
A program may use at most 128 MiB of HBM per device.

```python
import math
import jax
import jax.numpy as jnp
from jax import lax

GRID = 8192
VIS_DEV = 512
ROWS_DEV = 16
FACET_COLS = 4096
LAYERS = 8
GROUPS = 4
VIS = 16384
CAP = 32
FACET_ROWS = 128
N_WA = 8
N_CH = 4


def route_draw(key):
    blocks = VIS // VIS_DEV
    dest_count = LAYERS * GROUPS
    favoured = jax.random.randint(jax.random.fold_in(key, 11), (), 0, dest_count)

    def one_block(block_number):
        block_key = jax.random.fold_in(jax.random.fold_in(key, 13), block_number)
        order_key, share_key, shuffle_key = jax.random.split(block_key, 3)
        sequence = jax.random.permutation(order_key, dest_count).astype(jnp.int32)
        position_found = jnp.argmax(sequence == favoured)
        leading = sequence[0]
        sequence = sequence.at[position_found].set(leading).at[0].set(favoured)
        shares = jax.random.randint(share_key, (dest_count // 2,), 0, CAP + 1).at[0].set(CAP)
        paired = jnp.stack([shares, CAP - shares], 1).reshape(dest_count)
        counts = jnp.zeros((dest_count,), jnp.int32).at[sequence].set(paired.astype(jnp.int32))
        boundaries = jnp.cumsum(counts)
        position = jnp.arange(VIS_DEV, dtype=jnp.int32)
        destination = jnp.sum((position[:, None] >= boundaries[None, :]).astype(jnp.int32), 1)
        return jax.random.permutation(shuffle_key, destination)
    every = jax.vmap(one_block)(jnp.arange(blocks, dtype=jnp.int32))
    return every.reshape(VIS).astype(jnp.int32)


def draw_layer_index(key, part):
    return (route_draw(jax.random.fold_in(key, 7)) // GROUPS).astype(jnp.int32)


def draw_group_index(key, part):
    return (route_draw(jax.random.fold_in(key, 7)) % GROUPS).astype(jnp.int32)


def touch_ends(entries, rng, least, top_value):
    longest = entries.shape.index(max(entries.shape))
    spots = []
    for shift in (0, 1):
        where = [jax.random.randint(jax.random.fold_in(rng, axis), (), 0, length) for axis, length in enumerate(entries.shape)]
        where[longest] = (where[longest] + shift) % entries.shape[longest]
        spots.append(tuple(where))
    return entries.at[spots[0]].set(least).at[spots[1]].set(top_value)


def level_of(key, dims, shards, least, largest):
    loudness, own = 1.0, jax.random.fold_in(key, 6)
    for axis_at, blocks in shards:
        draws = jnp.exp(jax.random.uniform(jax.random.fold_in(own, axis_at), (blocks,), jnp.float32, least / len(shards), largest / len(shards)))
        loudness = loudness * jnp.repeat(draws, dims[axis_at] // blocks).reshape([-1 if axis == axis_at else 1 for axis in range(len(dims))])
    return loudness


def centred(own_key, shape, width, reach, cuts=(), kind=jnp.bfloat16):
    entries = width * jax.random.normal(own_key, shape, jnp.float32)
    if cuts:
        entries = entries * level_of(own_key, shape, cuts, -0.22, 0.18)
    return jnp.clip(entries, -reach, reach).astype(kind)


def setup_inputs(seed: int = 0) -> dict:
    arg_keys = jax.random.split(jax.random.key(seed), 8)
    grid_cells = touch_ends(jax.random.randint(arg_keys[0], (2, VIS), -(GRID // 2), GRID // 2), jax.random.fold_in(arg_keys[0], 1), -(GRID // 2), (GRID // 2) - 1).astype(jnp.int32)
    visibilities = centred(arg_keys[1], (2, VIS), 1.0, 6.0, ((1, 32),), jnp.float32)
    weights = jnp.clip(jnp.exp(math.log(4.0) - 2.7725887 * jax.random.uniform(arg_keys[2], (VIS,), jnp.float32) ** level_of(arg_keys[2], (VIS,), ((0, 32),), -0.2, 0.2)), 0.25, 4.0)
    layer_index = draw_layer_index(jax.random.fold_in(arg_keys[7], 71), 0)
    group_index = draw_group_index(jax.random.fold_in(arg_keys[7], 71), 0)
    plane_depths = jnp.clip(jax.random.uniform(arg_keys[5], (LAYERS,), jnp.float32, -1000.0, 1000.0) * level_of(arg_keys[5], (LAYERS,), ((0, 8),), -0.4, 0.0), -1000.0, 1000.0)
    sky_model = centred(arg_keys[6], (GROUPS, FACET_ROWS, FACET_COLS), 1.0, 6.0, ((0, 4), (1, 8)), jnp.float32)
    return dict(grid_cells=grid_cells, visibilities=visibilities, weights=weights, layer_index=layer_index, group_index=group_index, plane_depths=plane_depths, sky_model=sky_model)


def phase_table(left, right, grid_size):
    product = jnp.mod(left[:, None] * right[None, :], grid_size)
    return product.astype(jnp.float32) * (2.0 * math.pi / grid_size)

def column_factor(real_part, imag_part, weight, column_cells, columns, grid_size):
    pixels = jnp.arange(columns, dtype=jnp.int32) - columns // 2 + grid_size // 8
    angles = phase_table(column_cells, pixels, grid_size)
    weighted_real = weight * real_part
    weighted_imag = weight * imag_part
    cosines = jnp.cos(angles)
    sine_values = jnp.sin(angles)
    column_real = (weighted_real[:, None] * cosines - weighted_imag[:, None] * sine_values).astype(jnp.bfloat16)
    column_imag = (weighted_real[:, None] * sine_values + weighted_imag[:, None] * cosines).astype(jnp.bfloat16)
    return jnp.concatenate([column_real, column_imag], 0)

def row_factor(row_cells, row_start, row_count, total_rows, grid_size):
    pixels = row_start + jnp.arange(row_count, dtype=jnp.int32) - total_rows // 2 + grid_size // 8
    angles = phase_table(pixels, row_cells, grid_size)
    real_part = jnp.cos(angles).astype(jnp.bfloat16)
    imag_part = jnp.sin(angles).astype(jnp.bfloat16)
    upper_half = jnp.concatenate([real_part, -imag_part], 1)
    lower_half = jnp.concatenate([imag_part, real_part], 1)
    return jnp.concatenate([upper_half, lower_half], 0)

def layer_image(row_factors, column_factors, w_value, row_start, row_count, total_rows, columns, grid_size):
    product = jnp.dot(row_factors, column_factors, preferred_element_type=jnp.float32)
    real_sum = product[:row_count]
    imag_sum = product[row_count:]
    row_pixels = row_start + jnp.arange(row_count, dtype=jnp.int32) - total_rows // 2 + grid_size // 8
    column_pixels = jnp.arange(columns, dtype=jnp.int32) - columns // 2 + grid_size // 8
    row_cosine = 0.8 * row_pixels.astype(jnp.float32) / grid_size
    column_cosine = 0.8 * column_pixels.astype(jnp.float32) / grid_size
    depth_term = jnp.sqrt(1.0 - row_cosine[:, None] ** 2 - column_cosine[None, :] ** 2) - 1.0
    screen = 2.0 * math.pi * w_value * depth_term
    return jnp.cos(screen) * real_sum - jnp.sin(screen) * imag_sum

def reference(grid_cells, visibilities, weights, layer_index, group_index, plane_depths, sky_model):
    dest_count = N_WA * N_CH
    slot_count = CAP * N_WA * N_CH
    total_rows = ROWS_DEV * N_WA
    columns = FACET_COLS
    target = (layer_index * N_CH + group_index).astype(jnp.int32)
    sorting = jnp.argsort(target, stable=True)
    counts = jnp.bincount(target, length=dest_count).astype(jnp.int32)
    starts = (jnp.cumsum(counts) - counts).astype(jnp.int32)
    payload = jnp.stack([visibilities[0], visibilities[1], weights], 0)[:, sorting]
    payload = jnp.concatenate([payload, jnp.zeros((3, slot_count), payload.dtype)], 1)
    cells = grid_cells[:, sorting].astype(jnp.int32)
    cells = jnp.concatenate([cells, jnp.zeros((2, slot_count), jnp.int32)], 1)

    def add_dest(dirty_all, dest_number):
        offset_start = starts[dest_number]
        dest_data = lax.dynamic_slice_in_dim(payload, offset_start, slot_count, 1)
        dest_cells = lax.dynamic_slice_in_dim(cells, offset_start, slot_count, 1)
        live_mask = (jnp.arange(slot_count, dtype=jnp.int32) < counts[dest_number]).astype(dest_data.dtype)
        weight = dest_data[2] * live_mask
        column_factors = column_factor(dest_data[0], dest_data[1], weight, dest_cells[1], columns, GRID)
        row_factors = row_factor(dest_cells[0], jnp.int32(0), total_rows, total_rows, GRID)
        contribution = layer_image(row_factors, column_factors, plane_depths[dest_number // N_CH], jnp.int32(0), total_rows, total_rows, columns, GRID)
        target_group = dest_number % N_CH
        return (dirty_all.at[target_group].add(contribution), None)
    dirty_all, _ = lax.scan(add_dest, jnp.zeros((N_CH, total_rows, columns), jnp.float32), jnp.arange(dest_count, dtype=jnp.int32))
    member = (group_index[None, :] == jnp.arange(N_CH, dtype=jnp.int32)[:, None]).astype(jnp.float32)
    noise_power = lax.optimization_barrier(jnp.sum(member * (weights * weights)[None, :], 1))
    return dirty_all * lax.rsqrt(noise_power)[:, None, None] - sky_model
```

```python
import functools

import jax
import jax.numpy as jnp
from jax import lax
from jax.experimental import pallas as pl
from jax.experimental.pallas import tpu as pltpu
from jax.sharding import PartitionSpec as P

GRID = 8192
MESH = pl.DeviceIdType.MESH
SIN = (3.1415926400772034, -5.167710076668359, 2.5500773865296704, -0.5982904112879445, 0.07765591228493303)
COS = (0.9999999530275129, -4.934792802489486, 4.058410790762989, -1.3318729727896825, 0.21968242357961013)
F32 = jnp.float32
BF16 = jnp.bfloat16


def sincos(turns):
    y = turns * turns
    s = SIN[4]
    c = COS[4]
    for k in (3, 2, 1, 0):
        s = s * y + SIN[k]
        c = c * y + COS[k]
    s = s * turns
    s2 = s + s
    return s2 * c, 1.0 - s2 * s


def unit(phase):
    wrapped = ((phase + GRID) & (2 * GRID - 1)) - GRID
    return sincos(wrapped.astype(F32) * (0.5 / GRID))


def split3(x):
    high = x.astype(BF16)
    rest = x - high.astype(F32)
    mid = rest.astype(BF16)
    low = (rest - mid.astype(F32)).astype(BF16)
    return high, mid, low


def dot_nt(left, right):
    return lax.dot_general(left, right, (((1,), (1,)), ((), ())), preferred_element_type=F32)


def dot_nn(left, right):
    return jnp.dot(left, right, preferred_element_type=F32)


def exchange(axis, count, send_sem, recv_sem, source, target):
    me = lax.axis_index(axis)
    copies = []
    for step in range(1, count):
        to = lax.rem(me + step, count)
        copy = pltpu.make_async_remote_copy(
            src_ref=source(to),
            dst_ref=target(me),
            send_sem=send_sem.at[step],
            recv_sem=recv_sem.at[step],
            device_id={axis: to},
            device_id_type=MESH,
        )
        copy.start()
        copies.append(copy)
    return copies


def kernel(
    sizes, pay_ref, sky_ref, out_ref, msg, got, gathered, depth, a_ref, b_ref, x_ref, acc, outb, land,
    send1, recv1, send2, recv2, send3, recv3,
):
    n_wa, n_ch, cap, rows, rows_dev, columns = sizes
    layers = n_wa
    cols = columns // n_wa
    half_c, half_r = cols // 2, rows // 2
    held = pay_ref.shape[1]
    dests = n_wa * n_ch
    width = layers * cap
    me_wa, me_ch = lax.axis_index("wa"), lax.axis_index("ch")

    barrier = pltpu.get_barrier_semaphore()
    for axis, count, me in (("wa", n_wa, me_wa), ("ch", n_ch, me_ch)):
        for step in range(1, count):
            pl.semaphore_signal(
                barrier, inc=1, device_id={axis: lax.rem(me + step, count)}, device_id_type=MESH
            )

    payload = pay_ref[...]
    target = payload[5:6, :] * float(layers) + payload[6:7, :]
    onehot = lax.broadcasted_iota(jnp.int32, (dests, held), 0).astype(F32) == target
    earlier = (
        lax.broadcasted_iota(jnp.int32, (held, held), 0)
        < lax.broadcasted_iota(jnp.int32, (held, held), 1)
    )
    before = dot_nn(
        jnp.where(onehot, 1.0, 0.0).astype(BF16), jnp.where(earlier, 1.0, 0.0).astype(BF16)
    )
    rank = jnp.sum(jnp.where(onehot, before, 0.0), 0, keepdims=True)
    slot = target * float(cap) + rank
    parts = split3(payload)
    for group in range(n_ch):
        numbers = lax.broadcasted_iota(jnp.int32, (width, held), 0) + group * width
        select = jnp.where(numbers.astype(F32) == slot, 1.0, 0.0).astype(BF16)
        high, mid, low = (dot_nt(part, select) for part in parts)
        msg[group] = (high + mid) + low

    pl.semaphore_wait(barrier, n_wa + n_ch - 2)
    copies = exchange("ch", n_ch, send1, recv1, lambda to: msg.at[to], lambda me: got.at[me])
    got[me_ch] = msg[me_ch]

    left = me_wa * cols - columns // 2 + GRID // 8 + half_c
    top = GRID // 8

    @pl.loop(0, half_r // 8)
    def _(i):
        p = lax.broadcasted_iota(jnp.int32, (8, half_c), 0) + i * 8
        q = lax.broadcasted_iota(jnp.int32, (8, half_c), 1)
        for s1 in range(2):
            for s2 in range(2):
                l_pix = top + p if s1 == 0 else top - 1 - p
                m_pix = left + q if s2 == 0 else left - 1 - q
                l = 0.8 * l_pix.astype(F32) / GRID
                m = 0.8 * m_pix.astype(F32) / GRID
                s = l * l + m * m
                depth[2 * s1 + s2, pl.ds(i * 8, 8), :] = -s / (1.0 + jnp.sqrt(1.0 - s))
                acc[2 * s1 + s2, pl.ds(i * 8, 8), :] = jnp.zeros((8, half_c), F32)

    for copy in copies:
        copy.wait()

    lane = lax.broadcasted_iota(jnp.int32, (8, 128), 1)
    sub = lax.broadcasted_iota(jnp.int32, (8, 128), 0)

    def packed(layer):
        tile = jnp.zeros((8, 128), F32)
        at = layer * cap
        for c in range(n_ch):
            piece = got[c, :, at // 128 * 128 : at // 128 * 128 + 128]
            shift = (c * cap - at) % 128
            if shift:
                piece = pltpu.roll(piece, shift, 1)
            tile = jnp.where((lane >= c * cap) & (lane < (c + 1) * cap), piece, tile)
        return tile

    for pair in range(layers // 2):
        odd = pltpu.roll(packed(2 * pair + 1), 4, 0)
        gathered[me_wa, pair] = jnp.where(sub < 4, packed(2 * pair), odd)
    power = jnp.zeros((1, width), F32)
    for c in range(n_ch):
        weight = got[c, 4:5, :]
        power = power + weight * weight
    power = jnp.sum(power, 1, keepdims=True)
    gathered[me_wa, layers // 2] = jnp.where(sub == 0, payload[7:8, :128], jnp.where(sub == 1, power, 0.0))

    mine = gathered.at[me_wa]
    copies = exchange("wa", n_wa, send2, recv2, lambda to: mine, lambda me: gathered.at[me])
    for copy in copies:
        copy.wait()

    center_r = 2 * (GRID // 8) - 1
    center_c = 2 * left - 1
    f_iota = lax.broadcasted_iota(jnp.int32, (16, 128), 0) * 2 + 1

    def layer_step(pair, parity):
        @pl.loop(0, n_wa)
        def _(block):
            lanes = pl.ds(pl.multiple_of(block * 128, 128), 128)
            base = 4 * parity
            zr, zi = (gathered[block, pair, base + k : base + k + 1, :] for k in (0, 1))
            u, v = (gathered[block, pair, base + k : base + k + 1, :].astype(jnp.int32) for k in (2, 3))
            sc, cc = unit(u * center_r + v * center_c)
            wr, wi = zr * cc - zi * sc, zr * sc + zi * cc
            wr, wi = jnp.broadcast_to(wr, (16, 128)), jnp.broadcast_to(wi, (16, 128))
            for cell, half in ((u, half_r), (v, half_c)):
                fs, fc = unit(cell * f_iota)
                coarse = max(half // 16, 8)
                steps = lax.broadcasted_iota(jnp.int32, (coarse, 128), 0) * 32
                es, ec = unit(cell * steps)
                for a in range(half // 16):
                    e_s, e_c = es[a : a + 1, :], ec[a : a + 1, :]
                    c = e_c * fc - e_s * fs
                    s = e_s * fc + e_c * fs
                    if cell is u:
                        for k, term in enumerate((wr * c, wr * s, wi * c, wi * s)):
                            a_ref[k * half + 16 * a : k * half + 16 * a + 16, lanes] = term.astype(BF16)
                    else:
                        for k, term in enumerate((c, s)):
                            b_ref[k * half + 16 * a : k * half + 16 * a + 16, lanes] = term.astype(BF16)

        deep = min(1024, n_wa * 128)

        @pl.loop(0, 4 * half_r // 256)
        def _(i):
            tall = pl.ds(pl.multiple_of(i * 256, 256), 256)
            if n_wa * 128 == deep:
                x_ref[tall, :] = dot_nt(a_ref[tall, :], b_ref[...])
            else:
                x_ref[tall, :] = jnp.zeros((256, cols), F32)

                @pl.loop(0, n_wa * 128 // deep)
                def _(k):
                    inner = pl.ds(pl.multiple_of(k * deep, deep), deep)
                    x_ref[tall, :] += dot_nt(a_ref[tall, inner], b_ref[:, inner])

        w = gathered[2 * pair + parity, layers // 2, 0:1, 0:1]

        @pl.loop(0, half_r // 8)
        def _(i):
            x = [
                [
                    x_ref[pl.ds(pl.multiple_of(k * half_r + i * 8, 8), 8), g * half_c : (g + 1) * half_c]
                    for g in range(2)
                ]
                for k in range(4)
            ]
            (rcc, rcs), (rsc, rss), (icc, ics), (isc, iss) = x
            same_r, cross_r = (rcc - rss, rcc + rss), (isc + ics, isc - ics)
            same_i, cross_i = (icc - iss, icc + iss), (rsc + rcs, rsc - rcs)
            for s1 in range(2):
                for s2 in range(2):
                    k = 0 if s1 == s2 else 1
                    if s1 == 0:
                        real, imag = same_r[k] - cross_r[k], same_i[k] + cross_i[k]
                    else:
                        real, imag = same_r[k] + cross_r[k], same_i[k] - cross_i[k]
                    at = pl.ds(pl.multiple_of(i * 8, 8), 8)
                    turns = depth[2 * s1 + s2, at, :] * w
                    turns = turns - jnp.round(turns)
                    s, c = sincos(turns)
                    acc[2 * s1 + s2, at, :] += c * real - s * imag

    @pl.loop(0, layers // 2)
    def _(pair):
        for parity in range(2):
            layer_step(pair, parity)

    def mirror(n):
        one = lax.broadcasted_iota(jnp.int32, (n, n), 0)
        two = lax.broadcasted_iota(jnp.int32, (n, n), 1)
        return jnp.where(one + two == n - 1, 1.0, 0.0).astype(BF16)

    flip_c, flip_r = mirror(half_c), mirror(half_r)

    def wide(s1):
        high, mid, low = (dot_nn(part, flip_c) for part in split3(acc[2 * s1 + 1]))
        return jnp.concatenate([(high + mid) + low, acc[2 * s1]], 1)

    high, mid, low = (dot_nn(flip_r, part) for part in split3(wide(1)))
    blocks = half_r // rows_dev
    outb[:blocks] = ((high + mid) + low).reshape(blocks, rows_dev, cols)
    outb[blocks:] = wide(0).reshape(blocks, rows_dev, cols)

    copies = exchange("wa", n_wa, send3, recv3, lambda to: outb.at[to], lambda me: land.at[me])
    land[me_wa] = outb[me_wa]
    noise = jnp.zeros((1, 1), F32)
    for s in range(n_wa):
        noise = noise + gathered[s, layers // 2, 1:2, 0:1]
    scale = lax.rsqrt(noise)
    for copy in copies:
        copy.wait()
    for s in range(n_wa):
        span = slice(s * cols, (s + 1) * cols)
        out_ref[:, span] = land[s] * scale - sky_ref[:, span]


def on_device(grid_cells, visibilities, weights, layer_index, group_index, plane_depths, sky_model):
    n_wa, n_ch = lax.axis_size("wa"), lax.axis_size("ch")
    held = weights.shape[0]
    cap = 2 * held // (n_wa * n_ch)
    rows_dev, columns = sky_model.shape[1:]
    rows = rows_dev * n_wa
    cols = columns // n_wa
    payload = jnp.concatenate(
        [
            visibilities * weights[None],
            grid_cells.astype(F32),
            weights[None],
            group_index.astype(F32)[None],
            layer_index.astype(F32)[None],
            jnp.broadcast_to(plane_depths[None], (1, held)),
        ],
        0,
    )
    vmem = pl.BlockSpec(memory_space=pltpu.VMEM)
    out = pl.pallas_call(
        functools.partial(kernel, (n_wa, n_ch, cap, rows, rows_dev, columns)),
        out_shape=jax.ShapeDtypeStruct((rows_dev, columns), F32),
        in_specs=[vmem, vmem],
        out_specs=vmem,
        scratch_shapes=[
            pltpu.VMEM((n_ch, 8, n_wa * cap), F32),
            pltpu.VMEM((n_ch, 8, n_wa * cap), F32),
            pltpu.VMEM((n_wa, n_wa // 2 + 1, 8, 128), F32),
            pltpu.VMEM((4, rows // 2, cols // 2), F32),
            pltpu.VMEM((2 * rows, n_wa * 128), BF16),
            pltpu.VMEM((cols, n_wa * 128), BF16),
            pltpu.VMEM((2 * rows, cols), F32),
            pltpu.VMEM((4, rows // 2, cols // 2), F32),
            pltpu.VMEM((n_wa, rows_dev, cols), F32),
            pltpu.VMEM((n_wa, rows_dev, cols), F32),
        ]
        + [pltpu.SemaphoreType.DMA((n,)) for n in (n_ch, n_ch, n_wa, n_wa, n_wa, n_wa)],
        compiler_params=pltpu.CompilerParams(
            collective_id=0, has_side_effects=True, vmem_limit_bytes=48 * 1024 * 1024
        ),
    )(payload, sky_model[0])
    return out[None]


def solution(mesh):
    return jax.shard_map(
        on_device,
        mesh=mesh,
        in_specs=(
            P(None, ("wa", "ch")),
            P(None, ("wa", "ch")),
            P(("wa", "ch")),
            P(("wa", "ch")),
            P(("wa", "ch")),
            P("wa"),
            P("ch", "wa", None),
        ),
        out_specs=P("ch", "wa", None),
        check_vma=False,
    )
```

```python
import functools

import jax
import jax.numpy as jnp
from jax import lax
from jax.experimental import pallas as pl
from jax.experimental.pallas import tpu as pltpu
from jax.sharding import PartitionSpec as P

GRID = 8192
MESH = pl.DeviceIdType.MESH
SIN = (3.1415926400772034, -5.167710076668359, 2.5500773865296704, -0.5982904112879445, 0.07765591228493303)
COS = (0.9999999530275129, -4.934792802489486, 4.058410790762989, -1.3318729727896825, 0.21968242357961013)
F32 = jnp.float32
BF16 = jnp.bfloat16


def sincos(turns):
    y = turns * turns
    s = SIN[4]
    c = COS[4]
    for k in (3, 2, 1, 0):
        s = s * y + SIN[k]
        c = c * y + COS[k]
    s = s * turns
    s2 = s + s
    return s2 * c, 1.0 - s2 * s


def wrapped(turns):
    return turns - jnp.round(turns)


def across(index, step):
    moved = 0
    bit = 1
    while bit < 64:
        moved = moved + bit * lax.rem(lax.div(index, bit) + lax.div(step, bit), 2)
        bit *= 2
    return moved


def split3(x):
    high = x.astype(BF16)
    rest = x - high.astype(F32)
    mid = rest.astype(BF16)
    low = (rest - mid.astype(F32)).astype(BF16)
    return high, mid, low


def dot_nt(left, right):
    return lax.dot_general(left, right, (((1,), (1,)), ((), ())), preferred_element_type=F32)


def dot_nn(left, right):
    return jnp.dot(left, right, preferred_element_type=F32)


def remote(axis, step, send_sem, recv_sem, source, target):
    me = lax.axis_index(axis)
    to = across(me, jnp.int32(step))
    return pltpu.make_async_remote_copy(
        src_ref=source(to),
        dst_ref=target(me),
        send_sem=send_sem.at[step],
        recv_sem=recv_sem.at[step],
        device_id={axis: to},
        device_id_type=MESH,
    )


def kernel(
    sizes, cells_in, vis_in, weights_in, layer_in, group_in, depth_in, sky_in, out_ref,
    cells_ref, vis_ref, weights_ref, layer_ref, group_ref, sky_ref,
    msg, got, gathered, depth, a_ref, b_ref, x0_ref, x1_ref, acc, outb, land,
    in_sem, send1, recv1, send2, recv2, send3, recv3,
):
    n_wa, n_ch, cap, rows, rows_dev, columns = sizes
    layers = n_wa
    cols = columns // n_wa
    half_c, half_r = cols // 2, rows // 2
    held = weights_ref.shape[1]
    dests = n_wa * n_ch
    width = layers * cap
    resident = a_ref.shape[0] == layers
    me_wa, me_ch = lax.axis_index("wa"), lax.axis_index("ch")

    loads = [
        pltpu.make_async_copy(source, target, in_sem.at[k])
        for k, (source, target) in enumerate(
            (
                (layer_in, layer_ref), (group_in, group_ref), (weights_in, weights_ref),
                (vis_in, vis_ref), (cells_in, cells_ref), (sky_in, sky_ref),
            )
        )
    ]
    for load in loads:
        load.start()
    barrier = pltpu.get_barrier_semaphore()
    for axis, count, me in (("wa", n_wa, me_wa), ("ch", n_ch, me_ch)):
        for step in range(1, count):
            pl.semaphore_signal(
                barrier, inc=1, device_id={axis: across(me, jnp.int32(step))}, device_id_type=MESH
            )

    earlier = (
        lax.broadcasted_iota(jnp.int32, (held, held), 0)
        < lax.broadcasted_iota(jnp.int32, (held, held), 1)
    )
    earlier = jnp.where(earlier, 1.0, 0.0).astype(BF16)
    for load in loads[:-1]:
        load.wait()
    target = group_ref[...].astype(F32) * float(layers) + layer_ref[...].astype(F32)
    weights = weights_ref[...]
    payload = jnp.concatenate(
        [vis_ref[...] * weights, cells_ref[...].astype(F32), weights, jnp.zeros((3, held), F32)], 0
    )
    onehot = lax.broadcasted_iota(jnp.int32, (dests, held), 0).astype(F32) == target
    before = dot_nn(jnp.where(onehot, 1.0, 0.0).astype(BF16), earlier)
    rank = jnp.sum(jnp.where(onehot, before, 0.0), 0, keepdims=True)
    slot = target * float(cap) + rank
    parts = split3(payload)
    for group in range(n_ch):
        numbers = lax.broadcasted_iota(jnp.int32, (width, held), 0) + group * width
        select = jnp.where(numbers.astype(F32) == slot, 1.0, 0.0).astype(BF16)
        high, mid, low = (dot_nt(part, select) for part in parts)
        msg[group] = (high + mid) + low

    pl.semaphore_wait(barrier, n_wa + n_ch - 2)
    copies = [
        remote("ch", step, send1, recv1, lambda to: msg.at[to], lambda me: got.at[me])
        for step in range(1, n_ch)
    ]
    for copy in copies:
        copy.start()
    got[me_ch] = msg[me_ch]

    left = me_wa * cols - columns // 2 + GRID // 8 + half_c
    top = GRID // 8

    @pl.loop(0, half_r // 8)
    def _(i):
        p = lax.broadcasted_iota(jnp.int32, (8, half_c), 0) + i * 8
        q = lax.broadcasted_iota(jnp.int32, (8, half_c), 1)
        at = pl.ds(pl.multiple_of(i * 8, 8), 8)
        for s1 in range(2):
            for s2 in range(2):
                l_pix = top + p if s1 == 0 else top - 1 - p
                m_pix = left + q if s2 == 0 else left - 1 - q
                l = 0.8 * l_pix.astype(F32) / GRID
                m = 0.8 * m_pix.astype(F32) / GRID
                s = l * l + m * m
                depth[2 * s1 + s2, at, :] = -s / (1.0 + jnp.sqrt(1.0 - s))
                acc[2 * s1 + s2, at, :] = jnp.zeros((8, half_c), F32)

    for copy in copies:
        copy.wait()

    lane = lax.broadcasted_iota(jnp.int32, (8, 128), 1)
    sub = lax.broadcasted_iota(jnp.int32, (8, 128), 0)

    def packed(layer):
        tile = jnp.zeros((8, 128), F32)
        at = layer * cap
        for c in range(n_ch):
            piece = got[c, :, at // 128 * 128 : at // 128 * 128 + 128]
            shift = (c * cap - at) % 128
            if shift:
                piece = pltpu.roll(piece, shift, 1)
            tile = jnp.where((lane >= c * cap) & (lane < (c + 1) * cap), piece, tile)
        return tile

    for pair in range(layers // 2):
        odd = pltpu.roll(packed(2 * pair + 1), 4, 0)
        gathered[me_wa, pair] = jnp.where(sub < 4, packed(2 * pair), odd)
    power = jnp.zeros((1, width), F32)
    for c in range(n_ch):
        weight = got[c, 4:5, :]
        power = power + weight * weight
    power = jnp.sum(power, 1, keepdims=True)
    gathered[me_wa, layers // 2] = jnp.where(sub == 0, depth_in[0], jnp.where(sub == 1, power, 0.0))

    def spread(step):
        return remote("wa", step, send2, recv2, lambda to: gathered.at[me_wa], lambda me: gathered.at[me])

    for step in range(1, n_wa):
        spread(step).start()

    scale = 0.5 / GRID
    fine = (sub * 2 + 1).astype(F32) * scale
    coarse = (sub * 32).astype(F32) * scale
    center_c = 2 * left - 1
    center_high = lax.div(center_c + 2 * GRID, 64) - GRID // 32
    center_low = center_c - 64 * center_high
    center_high = center_high.astype(F32) * (64 * scale)
    center_low = center_low.astype(F32) * scale

    def rowwise(*values):
        tile = jnp.zeros((8, 128), F32)
        for row, value in values:
            tile = jnp.where(sub == row, value, tile)
        return tile

    mixed_u = rowwise((0, (GRID // 4 - 1) * scale), (1, 16 * scale), (3, 256 * scale))
    mixed_v = rowwise((0, center_high), (2, 16 * scale), (4, 256 * scale))
    mixed_low = rowwise((0, center_low))

    def times(first, second):
        (s1, c1), (s2, c2) = first, second
        return s1 * c2 + c1 * s2, c1 * c2 - s1 * s2

    def tables(block, pair, parity, held_at):
        lanes = pl.ds(pl.multiple_of(block * 128, 128), 128)
        base = 4 * parity
        zr, zi, u, v = (gathered[block, pair, base + k : base + k + 1, :] for k in range(4))
        ub, vb = jnp.broadcast_to(u, (8, 128)), jnp.broadcast_to(v, (8, 128))
        ms, mc = sincos(wrapped(wrapped(ub * mixed_u) + wrapped(vb * mixed_v) + vb * mixed_low))
        row = lambda k: (ms[k : k + 1, :], mc[k : k + 1, :])
        sc, cc = row(0)
        wr, wi = zr * cc - zi * sc, zr * sc + zi * cc
        wr, wi = jnp.broadcast_to(wr, (16, 128)), jnp.broadcast_to(wi, (16, 128))
        for cell, half, up, far in ((ub, half_r, 1, 3), (vb, half_c, 2, 4)):
            near = sincos(wrapped(cell * fine))
            upper = times(near, row(up))
            fs, fc = (jnp.concatenate([near[k], upper[k]], 0) for k in range(2))
            ladder = [sincos(wrapped(cell * coarse))]
            if half > 128:
                ladder.append(times(ladder[0], row(far)))
            for a in range(half // 16):
                es, ec = ladder[a // 8]
                e = es[a % 8 : a % 8 + 1, :], ec[a % 8 : a % 8 + 1, :]
                s, c = times(e, (fs, fc))
                if up == 1:
                    for k, term in enumerate((wr * c, wr * s, wi * c, wi * s)):
                        a_ref[held_at, k * half + 16 * a : k * half + 16 * a + 16, lanes] = term.astype(BF16)
                else:
                    for k, term in enumerate((c, s)):
                        b_ref[held_at, k * half + 16 * a : k * half + 16 * a + 16, lanes] = term.astype(BF16)

    def products(held_at, x_ref):
        deep = min(1024, n_wa * 128)
        for i in range(4 * half_r // 256):
            tall = slice(i * 256, i * 256 + 256)
            if n_wa * 128 == deep:
                x_ref[tall, :] = dot_nt(a_ref[held_at, tall, :], b_ref[held_at])
            else:
                x_ref[tall, :] = jnp.zeros((256, cols), F32)

                @pl.loop(0, n_wa * 128 // deep)
                def _(k):
                    inner = pl.ds(pl.multiple_of(k * deep, deep), deep)
                    x_ref[tall, :] += dot_nt(a_ref[held_at, tall, inner], b_ref[held_at, :, inner])

    def screened(x_ref, layer, i):
        w = gathered[layer, layers // 2, 0:1, 0:1]
        x = [
            [x_ref[k * half_r + i * 8 : k * half_r + i * 8 + 8, g * half_c : (g + 1) * half_c] for g in range(2)]
            for k in range(4)
        ]
        (rcc, rcs), (rsc, rss), (icc, ics), (isc, iss) = x
        same_r, cross_r = (rcc - rss, rcc + rss), (isc + ics, isc - ics)
        same_i, cross_i = (icc - iss, icc + iss), (rsc + rcs, rsc - rcs)
        at = slice(i * 8, i * 8 + 8)
        for s1 in range(2):
            for s2 in range(2):
                k = 0 if s1 == s2 else 1
                if s1 == 0:
                    real, imag = same_r[k] - cross_r[k], same_i[k] + cross_i[k]
                else:
                    real, imag = same_r[k] + cross_r[k], same_i[k] - cross_i[k]
                s, c = sincos(wrapped(depth[2 * s1 + s2, at, :] * w))
                acc[2 * s1 + s2, at, :] += c * real - s * imag

    def screen(x_ref, layer):
        for i in range(half_r // 8):
            screened(x_ref, layer, i)

    if resident:

        @pl.loop(0, n_wa)
        def _(step):
            @pl.when(step > 0)
            def _():
                spread(step).wait_recv()

            block = across(me_wa, step)

            @pl.loop(0, layers // 2)
            def _(pair):
                for parity in range(2):
                    tables(block, pair, parity, 2 * pair + parity)

        x1_ref[...] = jnp.zeros_like(x1_ref)

        @pl.loop(0, layers // 2)
        def _(pair):
            products(2 * pair, x0_ref)
            screen(x1_ref, jnp.maximum(2 * pair - 1, 0))
            products(2 * pair + 1, x1_ref)
            screen(x0_ref, 2 * pair)

        screen(x1_ref, layers - 1)
    else:
        for step in range(1, n_wa):
            spread(step).wait_recv()

        @pl.loop(0, layers // 2)
        def _(pair):
            for parity in range(2):

                @pl.loop(0, n_wa)
                def _(block):
                    tables(block, pair, parity, 0)

                products(0, x0_ref)
                screen(x0_ref, 2 * pair + parity)

    def mirror(n):
        one = lax.broadcasted_iota(jnp.int32, (n, n), 0)
        two = lax.broadcasted_iota(jnp.int32, (n, n), 1)
        return jnp.where(one + two == n - 1, 1.0, 0.0).astype(BF16)

    flip_c, flip_r = mirror(half_c), mirror(half_r)

    def wide(s1):
        high, mid, low = (dot_nn(part, flip_c) for part in split3(acc[2 * s1 + 1]))
        return jnp.concatenate([(high + mid) + low, acc[2 * s1]], 1)

    high, mid, low = (dot_nn(flip_r, part) for part in split3(wide(1)))
    blocks = half_r // rows_dev
    outb[:blocks] = ((high + mid) + low).reshape(blocks, rows_dev, cols)
    outb[blocks:] = wide(0).reshape(blocks, rows_dev, cols)

    copies = [
        remote("wa", step, send3, recv3, lambda to: outb.at[to], lambda me: land.at[me])
        for step in range(1, n_wa)
    ]
    for copy in reversed(copies):
        copy.start()
    land[me_wa] = outb[me_wa]
    noise = jnp.zeros((1, 1), F32)
    for s in range(n_wa):
        noise = noise + gathered[s, layers // 2, 1:2, 0:1]
    factor = lax.rsqrt(noise)
    for step in range(1, n_wa):
        spread(step).wait_send()
    loads[-1].wait()
    for copy in copies:
        copy.wait()
    for s in range(n_wa):
        span = slice(s * cols, (s + 1) * cols)
        out_ref[:, span] = land[s] * factor - sky_ref[:, span]


def on_device(grid_cells, visibilities, weights, layer_index, group_index, plane_depths, sky_model):
    n_wa, n_ch = lax.axis_size("wa"), lax.axis_size("ch")
    held = weights.shape[0]
    cap = 2 * held // (n_wa * n_ch)
    rows_dev, columns = sky_model.shape[1:]
    rows = rows_dev * n_wa
    cols = columns // n_wa
    depth = n_wa * 128
    table = 2 * (2 * rows + cols) * depth
    kept = n_wa if n_wa * table <= 16 * 1024 * 1024 else 1
    vmem = pl.BlockSpec(memory_space=pltpu.VMEM)
    hbm = pl.BlockSpec(memory_space=pltpu.HBM)
    smem = pl.BlockSpec(memory_space=pltpu.SMEM)
    out = pl.pallas_call(
        functools.partial(kernel, (n_wa, n_ch, cap, rows, rows_dev, columns)),
        out_shape=jax.ShapeDtypeStruct((rows_dev, columns), F32),
        in_specs=[hbm, hbm, hbm, hbm, hbm, smem, hbm],
        out_specs=vmem,
        scratch_shapes=[
            pltpu.VMEM((2, held), jnp.int32),
            pltpu.VMEM((2, held), F32),
            pltpu.VMEM((1, held), F32),
            pltpu.VMEM((1, held), jnp.int32),
            pltpu.VMEM((1, held), jnp.int32),
            pltpu.VMEM((rows_dev, columns), F32),
            pltpu.VMEM((n_ch, 8, n_wa * cap), F32),
            pltpu.VMEM((n_ch, 8, n_wa * cap), F32),
            pltpu.VMEM((n_wa, n_wa // 2 + 1, 8, 128), F32),
            pltpu.VMEM((4, rows // 2, cols // 2), F32),
            pltpu.VMEM((kept, 2 * rows, depth), BF16),
            pltpu.VMEM((kept, cols, depth), BF16),
            pltpu.VMEM((2 * rows, cols), F32),
            pltpu.VMEM((2 * rows, cols), F32),
            pltpu.VMEM((4, rows // 2, cols // 2), F32),
            pltpu.VMEM((n_wa, rows_dev, cols), F32),
            pltpu.VMEM((n_wa, rows_dev, cols), F32),
        ]
        + [pltpu.SemaphoreType.DMA((n,)) for n in (6, n_ch, n_ch, n_wa, n_wa, n_wa, n_wa)],
        compiler_params=pltpu.CompilerParams(
            collective_id=0, has_side_effects=True, vmem_limit_bytes=36 * 1024 * 1024
        ),
    )(
        grid_cells, visibilities, weights[None], layer_index[None], group_index[None],
        plane_depths, sky_model[0],
    )
    return out[None]


def solution(mesh):
    return jax.shard_map(
        on_device,
        mesh=mesh,
        in_specs=(
            P(None, ("wa", "ch")),
            P(None, ("wa", "ch")),
            P(("wa", "ch")),
            P(("wa", "ch")),
            P(("wa", "ch")),
            P("wa"),
            P("ch", "wa", None),
        ),
        out_specs=P("ch", "wa", None),
        check_vma=False,
    )
```

```python
import functools

import jax
import jax.numpy as jnp
from jax import lax
from jax.experimental import pallas as pl
from jax.experimental.pallas import tpu as pltpu
from jax.sharding import PartitionSpec as P

GRID = 8192
MESH = pl.DeviceIdType.MESH
SIN = (3.1415926400772034, -5.167710076668359, 2.5500773865296704, -0.5982904112879445, 0.07765591228493303)
COS = (0.9999999530275129, -4.934792802489486, 4.058410790762989, -1.3318729727896825, 0.21968242357961013)
F32 = jnp.float32
BF16 = jnp.bfloat16


def sincos(turns):
    y = turns * turns
    s = SIN[4]
    c = COS[4]
    for k in (3, 2, 1, 0):
        s = s * y + SIN[k]
        c = c * y + COS[k]
    s = s * turns
    s2 = s + s
    return s2 * c, 1.0 - s2 * s


def wrapped(turns):
    return turns - jnp.round(turns)


def across(index, step):
    moved = 0
    bit = 1
    while bit < 64:
        moved = moved + bit * lax.rem(lax.div(index, bit) + lax.div(step, bit), 2)
        bit *= 2
    return moved


def split3(x):
    high = x.astype(BF16)
    rest = x - high.astype(F32)
    mid = rest.astype(BF16)
    low = (rest - mid.astype(F32)).astype(BF16)
    return high, mid, low


def dot_nt(left, right):
    return lax.dot_general(left, right, (((1,), (1,)), ((), ())), preferred_element_type=F32)


def dot_nn(left, right):
    return jnp.dot(left, right, preferred_element_type=F32)


def remote(axis, step, send_sem, recv_sem, source, target):
    me = lax.axis_index(axis)
    to = across(me, jnp.int32(step))
    return pltpu.make_async_remote_copy(
        src_ref=source(to),
        dst_ref=target(me),
        send_sem=send_sem.at[step],
        recv_sem=recv_sem.at[step],
        device_id={axis: to},
        device_id_type=MESH,
    )


def kernel(
    sizes, cells_in, vis_in, weights_in, layer_in, group_in, depth_in, sky_in, out_ref,
    cells_ref, vis_ref, weights_ref, layer_ref, group_ref, sky_ref,
    msg, got, gathered, depth, a_ref, b_ref, x0_ref, x1_ref, acc, outb, land,
    in_sem, send1, recv1, send2, recv2, send3, recv3,
):
    n_wa, n_ch, cap, rows, rows_dev, columns = sizes
    layers = n_wa
    cols = columns // n_wa
    half_c, half_r = cols // 2, rows // 2
    chunks = outb.shape[0]
    chunk = half_c // chunks
    held = weights_ref.shape[1]
    dests = n_wa * n_ch
    width = layers * cap
    resident = a_ref.shape[0] == layers
    me_wa, me_ch = lax.axis_index("wa"), lax.axis_index("ch")

    loads = [
        pltpu.make_async_copy(source, target, in_sem.at[k])
        for k, (source, target) in enumerate(
            (
                (layer_in, layer_ref), (group_in, group_ref), (weights_in, weights_ref),
                (vis_in, vis_ref), (cells_in, cells_ref), (sky_in, sky_ref),
            )
        )
    ]
    for load in loads:
        load.start()
    barrier = pltpu.get_barrier_semaphore()
    for axis, count, me in (("wa", n_wa, me_wa), ("ch", n_ch, me_ch)):
        for step in range(1, count):
            pl.semaphore_signal(
                barrier, inc=1, device_id={axis: across(me, jnp.int32(step))}, device_id_type=MESH
            )

    earlier = (
        lax.broadcasted_iota(jnp.int32, (held, held), 0)
        < lax.broadcasted_iota(jnp.int32, (held, held), 1)
    )
    earlier = jnp.where(earlier, 1.0, 0.0).astype(BF16)
    for load in loads[:-1]:
        load.wait()
    target = group_ref[...].astype(F32) * float(layers) + layer_ref[...].astype(F32)
    weights = weights_ref[...]
    payload = jnp.concatenate(
        [vis_ref[...] * weights, cells_ref[...].astype(F32), weights, jnp.zeros((3, held), F32)], 0
    )
    onehot = lax.broadcasted_iota(jnp.int32, (dests, held), 0).astype(F32) == target
    before = dot_nn(jnp.where(onehot, 1.0, 0.0).astype(BF16), earlier)
    rank = jnp.sum(jnp.where(onehot, before, 0.0), 0, keepdims=True)
    slot = target * float(cap) + rank
    parts = split3(payload)
    for group in range(n_ch):
        numbers = lax.broadcasted_iota(jnp.int32, (width, held), 0) + group * width
        select = jnp.where(numbers.astype(F32) == slot, 1.0, 0.0).astype(BF16)
        high, mid, low = (dot_nt(part, select) for part in parts)
        msg[group] = (high + mid) + low

    pl.semaphore_wait(barrier, n_wa + n_ch - 2)
    copies = [
        remote("ch", step, send1, recv1, lambda to: msg.at[to], lambda me: got.at[me])
        for step in range(1, n_ch)
    ]
    for copy in copies:
        copy.start()
    got[me_ch] = msg[me_ch]

    left = me_wa * cols - columns // 2 + GRID // 8 + half_c
    top = GRID // 8

    @pl.loop(0, half_r // 8)
    def _(i):
        p = lax.broadcasted_iota(jnp.int32, (8, half_c), 0) + i * 8
        q = lax.broadcasted_iota(jnp.int32, (8, half_c), 1)
        at = pl.ds(pl.multiple_of(i * 8, 8), 8)
        for s1 in range(2):
            for s2 in range(2):
                l_pix = top + p if s1 == 0 else top - 1 - p
                m_pix = left + q if s2 == 0 else left - 1 - q
                l = 0.8 * l_pix.astype(F32) / GRID
                m = 0.8 * m_pix.astype(F32) / GRID
                s = l * l + m * m
                depth[2 * s1 + s2, at, :] = -s / (1.0 + jnp.sqrt(1.0 - s))
                acc[2 * s1 + s2, at, :] = jnp.zeros((8, half_c), F32)

    for copy in copies:
        copy.wait()

    lane = lax.broadcasted_iota(jnp.int32, (8, 128), 1)
    sub = lax.broadcasted_iota(jnp.int32, (8, 128), 0)

    def packed(layer):
        tile = jnp.zeros((8, 128), F32)
        at = layer * cap
        for c in range(n_ch):
            piece = got[c, :, at // 128 * 128 : at // 128 * 128 + 128]
            shift = (c * cap - at) % 128
            if shift:
                piece = pltpu.roll(piece, shift, 1)
            tile = jnp.where((lane >= c * cap) & (lane < (c + 1) * cap), piece, tile)
        return tile

    for pair in range(layers // 2):
        odd = pltpu.roll(packed(2 * pair + 1), 4, 0)
        gathered[me_wa, pair] = jnp.where(sub < 4, packed(2 * pair), odd)
    power = jnp.zeros((1, width), F32)
    for c in range(n_ch):
        weight = got[c, 4:5, :]
        power = power + weight * weight
    power = jnp.sum(power, 1, keepdims=True)
    gathered[me_wa, layers // 2] = jnp.where(sub == 0, depth_in[0], jnp.where(sub == 1, power, 0.0))

    def spread(step):
        return remote("wa", step, send2, recv2, lambda to: gathered.at[me_wa], lambda me: gathered.at[me])

    for step in range(1, n_wa):
        spread(step).start()

    scale = 0.5 / GRID
    fine = (sub * 2 + 1).astype(F32) * scale
    coarse = (sub * 32).astype(F32) * scale
    center_c = 2 * left - 1
    center_high = lax.div(center_c + 2 * GRID, 64) - GRID // 32
    center_low = center_c - 64 * center_high
    center_high = center_high.astype(F32) * (64 * scale)
    center_low = center_low.astype(F32) * scale

    def rowwise(*values):
        tile = jnp.zeros((8, 128), F32)
        for row, value in values:
            tile = jnp.where(sub == row, value, tile)
        return tile

    mixed_u = rowwise((0, (GRID // 4 - 1) * scale), (1, 16 * scale), (3, 256 * scale))
    mixed_v = rowwise((0, center_high), (2, 16 * scale), (4, 256 * scale))
    mixed_low = rowwise((0, center_low))

    def times(first, second):
        (s1, c1), (s2, c2) = first, second
        return s1 * c2 + c1 * s2, c1 * c2 - s1 * s2

    def tables(block, pair, parity, held_at):
        lanes = pl.ds(pl.multiple_of(block * 128, 128), 128)
        base = 4 * parity
        zr, zi, u, v = (gathered[block, pair, base + k : base + k + 1, :] for k in range(4))
        ub, vb = jnp.broadcast_to(u, (8, 128)), jnp.broadcast_to(v, (8, 128))
        ms, mc = sincos(wrapped(wrapped(ub * mixed_u) + wrapped(vb * mixed_v) + vb * mixed_low))
        row = lambda k: (ms[k : k + 1, :], mc[k : k + 1, :])
        sc, cc = row(0)
        wr, wi = zr * cc - zi * sc, zr * sc + zi * cc
        wr, wi = jnp.broadcast_to(wr, (16, 128)), jnp.broadcast_to(wi, (16, 128))
        for cell, half, up, far in ((ub, half_r, 1, 3), (vb, half_c, 2, 4)):
            near = sincos(wrapped(cell * fine))
            upper = times(near, row(up))
            fs, fc = (jnp.concatenate([near[k], upper[k]], 0) for k in range(2))
            ladder = [sincos(wrapped(cell * coarse))]
            if half > 128:
                ladder.append(times(ladder[0], row(far)))
            for a in range(half // 16):
                es, ec = ladder[a // 8]
                e = es[a % 8 : a % 8 + 1, :], ec[a % 8 : a % 8 + 1, :]
                s, c = times(e, (fs, fc))
                if up == 1:
                    for k, term in enumerate((wr * c, wr * s, wi * c, wi * s)):
                        a_ref[held_at, k * half + 16 * a : k * half + 16 * a + 16, lanes] = term.astype(BF16)
                else:
                    at = 2 * chunk * (16 * a // chunk) + 16 * a % chunk
                    for k, term in enumerate((c, s)):
                        b_ref[held_at, at + k * chunk : at + k * chunk + 16, lanes] = term.astype(BF16)

    def products(held_at, x_ref, h):
        deep = min(1024, n_wa * 128)
        across_h = slice(2 * chunk * h, 2 * chunk * (h + 1))
        for i in range(4 * half_r // 256):
            tall = slice(i * 256, i * 256 + 256)
            if n_wa * 128 == deep:
                x_ref[tall, :] = dot_nt(a_ref[held_at, tall, :], b_ref[held_at, across_h, :])
            else:
                x_ref[tall, :] = jnp.zeros((256, 2 * chunk), F32)

                @pl.loop(0, n_wa * 128 // deep)
                def _(k):
                    inner = pl.ds(pl.multiple_of(k * deep, deep), deep)
                    x_ref[tall, :] += dot_nt(a_ref[held_at, tall, inner], b_ref[held_at, across_h, inner])

    def screen(x_ref, layer, h):
        w = gathered[layer, layers // 2, 0:1, 0:1]
        wide_at = slice(chunk * h, chunk * (h + 1))
        for i in range(half_r // 8):
            x = [
                [x_ref[k * half_r + i * 8 : k * half_r + i * 8 + 8, g * chunk : (g + 1) * chunk] for g in range(2)]
                for k in range(4)
            ]
            (rcc, rcs), (rsc, rss), (icc, ics), (isc, iss) = x
            same_r, cross_r = (rcc - rss, rcc + rss), (isc + ics, isc - ics)
            same_i, cross_i = (icc - iss, icc + iss), (rsc + rcs, rsc - rcs)
            at = slice(i * 8, i * 8 + 8)
            for s1 in range(2):
                for s2 in range(2):
                    k = 0 if s1 == s2 else 1
                    if s1 == 0:
                        real, imag = same_r[k] - cross_r[k], same_i[k] + cross_i[k]
                    else:
                        real, imag = same_r[k] + cross_r[k], same_i[k] - cross_i[k]
                    s, c = sincos(wrapped(depth[2 * s1 + s2, at, wide_at] * w))
                    acc[2 * s1 + s2, at, wide_at] += c * real - s * imag

    def mirror(n):
        one = lax.broadcasted_iota(jnp.int32, (n, n), 0)
        two = lax.broadcasted_iota(jnp.int32, (n, n), 1)
        return jnp.where(one + two == n - 1, 1.0, 0.0).astype(BF16)

    flip_c, flip_r = mirror(chunk), mirror(half_r)
    blocks = half_r // rows_dev

    def wide(s1, h):
        wide_at = slice(chunk * h, chunk * (h + 1))
        high, mid, low = (dot_nn(part, flip_c) for part in split3(acc[2 * s1 + 1, :, wide_at]))
        return jnp.concatenate([(high + mid) + low, acc[2 * s1, :, wide_at]], 1)

    def owned(h):
        return [
            remote("wa", step, send3.at[h], recv3.at[h], lambda to: outb.at[h, to], lambda me: land.at[h, me])
            for step in range(1, n_wa)
        ]

    def hand_over(h):
        high, mid, low = (dot_nn(flip_r, part) for part in split3(wide(1, h)))
        outb[h, :blocks] = ((high + mid) + low).reshape(blocks, rows_dev, 2 * chunk)
        outb[h, blocks:] = wide(0, h).reshape(blocks, rows_dev, 2 * chunk)
        for copy in reversed(owned(h)):
            copy.start()
        land[h, me_wa] = outb[h, me_wa]

    if resident:

        @pl.loop(0, n_wa)
        def _(step):
            @pl.when(step > 0)
            def _():
                spread(step).wait_recv()

            block = across(me_wa, step)

            @pl.loop(0, layers // 2)
            def _(pair):
                for parity in range(2):
                    tables(block, pair, parity, 2 * pair + parity)

        for h in range(chunks):
            x1_ref[...] = jnp.zeros_like(x1_ref)

            @pl.loop(0, layers // 2)
            def _(pair):
                products(2 * pair, x0_ref, h)
                screen(x1_ref, jnp.maximum(2 * pair - 1, 0), h)
                products(2 * pair + 1, x1_ref, h)
                screen(x0_ref, 2 * pair, h)

            screen(x1_ref, layers - 1, h)
            hand_over(h)
    else:
        for step in range(1, n_wa):
            spread(step).wait_recv()

        @pl.loop(0, layers // 2)
        def _(pair):
            for parity in range(2):

                @pl.loop(0, n_wa)
                def _(block):
                    tables(block, pair, parity, 0)

                for h in range(chunks):
                    products(0, x0_ref, h)
                    screen(x0_ref, 2 * pair + parity, h)

        for h in range(chunks):
            hand_over(h)

    noise = jnp.zeros((1, 1), F32)
    for s in range(n_wa):
        noise = noise + gathered[s, layers // 2, 1:2, 0:1]
    factor = lax.rsqrt(noise)
    for step in range(1, n_wa):
        spread(step).wait_send()
    loads[-1].wait()
    for h in range(chunks):
        for copy in owned(h):
            copy.wait()
        for s in range(n_wa):
            minus = s * cols + half_c - chunk * (h + 1)
            plus = s * cols + half_c + chunk * h
            if chunk % 128:
                span = slice(s * cols, (s + 1) * cols)
                out_ref[:, span] = land[h, s] * factor - sky_ref[:, span]
            else:
                for k, at in enumerate((minus, plus)):
                    span = slice(at, at + chunk)
                    out_ref[:, span] = land[h, s, :, k * chunk : (k + 1) * chunk] * factor - sky_ref[:, span]


def on_device(grid_cells, visibilities, weights, layer_index, group_index, plane_depths, sky_model):
    n_wa, n_ch = lax.axis_size("wa"), lax.axis_size("ch")
    held = weights.shape[0]
    cap = 2 * held // (n_wa * n_ch)
    rows_dev, columns = sky_model.shape[1:]
    rows = rows_dev * n_wa
    cols = columns // n_wa
    depth = n_wa * 128
    table = 2 * (2 * rows + cols) * depth
    kept = n_wa if n_wa * table <= 16 * 1024 * 1024 else 1
    chunks = max(1, cols // 256)
    vmem = pl.BlockSpec(memory_space=pltpu.VMEM)
    hbm = pl.BlockSpec(memory_space=pltpu.HBM)
    smem = pl.BlockSpec(memory_space=pltpu.SMEM)
    out = pl.pallas_call(
        functools.partial(kernel, (n_wa, n_ch, cap, rows, rows_dev, columns)),
        out_shape=jax.ShapeDtypeStruct((rows_dev, columns), F32),
        in_specs=[hbm, hbm, hbm, hbm, hbm, smem, hbm],
        out_specs=vmem,
        scratch_shapes=[
            pltpu.VMEM((2, held), jnp.int32),
            pltpu.VMEM((2, held), F32),
            pltpu.VMEM((1, held), F32),
            pltpu.VMEM((1, held), jnp.int32),
            pltpu.VMEM((1, held), jnp.int32),
            pltpu.VMEM((rows_dev, columns), F32),
            pltpu.VMEM((n_ch, 8, n_wa * cap), F32),
            pltpu.VMEM((n_ch, 8, n_wa * cap), F32),
            pltpu.VMEM((n_wa, n_wa // 2 + 1, 8, 128), F32),
            pltpu.VMEM((4, rows // 2, cols // 2), F32),
            pltpu.VMEM((kept, 2 * rows, depth), BF16),
            pltpu.VMEM((kept, cols, depth), BF16),
            pltpu.VMEM((2 * rows, cols // chunks), F32),
            pltpu.VMEM((2 * rows, cols // chunks), F32),
            pltpu.VMEM((4, rows // 2, cols // 2), F32),
            pltpu.VMEM((chunks, n_wa, rows_dev, cols // chunks), F32),
            pltpu.VMEM((chunks, n_wa, rows_dev, cols // chunks), F32),
        ]
        + [pltpu.SemaphoreType.DMA((n,)) for n in (6, n_ch, n_ch, n_wa, n_wa)]
        + [pltpu.SemaphoreType.DMA((chunks, n_wa))] * 2,
        compiler_params=pltpu.CompilerParams(
            collective_id=0, has_side_effects=True, vmem_limit_bytes=56 * 1024 * 1024
        ),
    )(
        grid_cells, visibilities, weights[None], layer_index[None], group_index[None],
        plane_depths, sky_model[0],
    )
    return out[None]


def solution(mesh):
    return jax.shard_map(
        on_device,
        mesh=mesh,
        in_specs=(
            P(None, ("wa", "ch")),
            P(None, ("wa", "ch")),
            P(("wa", "ch")),
            P(("wa", "ch")),
            P(("wa", "ch")),
            P("wa"),
            P("ch", "wa", None),
        ),
        out_specs=P("ch", "wa", None),
        check_vma=False,
    )
```
